32 devices in a mesh: dp: 8 (over y, x, core), mp: 4 (over z).
Axes of the slice: x: 2, y: 2, z: 4, core: 2. Of those that a mesh axis runs over, the one named last changes fastest.
Arguments:
- hidden_states: bfloat16 [16384, 4096], P('dp', 'mp'), may hold values from -1 to 1
- factor_values: bfloat16 [16384, 64], P('dp', 'mp'), may hold values from 0.029907227 to 0.13964844
- class_ids: int32 [16384, 64], P('dp', 'mp'), may hold values from 0 to 128255, as said below
- centers: int32 [3], replicated, may hold values from 0 to 16383
Outputs:
- min_distance: float32 [16384], P(('dp', 'mp'))
- weight_means: float32 [3], replicated
The draws below stay inside these ranges and needn't reach their ends.
Inputs may be any that keep to these rules, and one draw needn't show every extreme that they name: `centers`: each value is a sample index. `class_ids`: entries k * 16 to (k + 1) * 16 - 1 of a row hold distinct classes of the k-th of 4 equal ranges of the vocabulary.
All inputs are finite; a program needn't handle non-finite values.
Results may differ from the reference program's by a relative error of at most 0.00095.
Values may be sent and summed in bfloat16 or wider, within the bound.
A program may use at most 64 MiB of HBM per device.

```python
import jax
import jax.numpy as jnp
from jax import lax

D = 4096
VOCAB = 128256
K_LOC = 16
STEPS = 3
SAMP_DEV = 512
TOPK = 64
POOL = 16384


def draw_hidden_states(key, part):
    key_shared, key_noise = jax.random.split(key, 2)
    shared = jax.random.normal(key_shared, (1, D), jnp.float32)
    noise = jax.random.normal(key_noise, (POOL, D), jnp.float32)
    base = 0.7 * shared + 0.7 * noise
    return jnp.clip(base / jnp.sqrt(jnp.float32(D)), -1.0, 1.0).astype(jnp.bfloat16)


def draw_class_ids(key, part):
    nblk = TOPK // K_LOC
    span = VOCAB // nblk
    stride = span // K_LOC
    key_order, key_pick, key_near, key_far = jax.random.split(key, 4)
    scores = jax.random.randint(key_order, (POOL, nblk, K_LOC), 0, 1 << 20) * K_LOC + jnp.arange(K_LOC, dtype=jnp.int32)
    slots = jnp.argsort(scores, axis=-1, stable=True).astype(jnp.int32)
    pick = jax.random.randint(key_pick, (POOL, nblk, K_LOC), 0, 4)
    near = jax.random.randint(key_near, (POOL, nblk, K_LOC), 0, 4)
    far = jax.random.randint(key_far, (POOL, nblk, K_LOC), 0, stride)
    offset = jnp.where(pick > 0, near, far)
    base = (jnp.arange(nblk, dtype=jnp.int32) * span).reshape(1, nblk, 1)
    ids = base + slots * stride + offset
    return ids.reshape(POOL, TOPK).astype(jnp.int32)


def levels(own_key, shape, cuts, smallest, high):
    level, own = 1.0, jax.random.fold_in(own_key, 6)
    for dim, shards_of in cuts:
        heights = jnp.exp(jax.random.uniform(jax.random.fold_in(own, dim), (shards_of,), jnp.float32, smallest / len(cuts), high / len(cuts)))
        level = level * jnp.repeat(heights, shape[dim] // shards_of).reshape([-1 if axis == dim else 1 for axis in range(len(shape))])
    return level


def setup_inputs(seed: int = 0) -> dict:
    key_list = jax.random.split(jax.random.key(seed), 5)
    hidden_states = draw_hidden_states(jax.random.fold_in(key_list[4], 71), 0)
    factor_values = jnp.clip(0.029907227 + 0.10974121 * jax.random.uniform(key_list[1], (POOL, TOPK), jnp.float32) ** levels(key_list[1], (POOL, TOPK), ((0, 8), (1, 4)), -0.2, 0.2), 0.029907227, 0.13964844).astype(jnp.bfloat16)
    class_ids = draw_class_ids(jax.random.fold_in(key_list[4], 71), 0)
    centers = jax.random.randint(key_list[3], (STEPS,), 0, POOL).astype(jnp.int32)
    return {"hidden_states": hidden_states, "factor_values": factor_values, "class_ids": class_ids, "centers": centers}


def reference(hidden_states, factor_values, class_ids, centers):
    nblk = TOPK // K_LOC
    vals = factor_values.astype(jnp.float32)
    sq_h = jnp.sum(jnp.square(hidden_states.astype(jnp.float32)), axis=1)
    sq_a = jnp.sum(vals * vals, axis=1)
    groups = POOL // SAMP_DEV
    means = []
    min_distance = None
    for step in range(STEPS):
        center = centers[step].astype(jnp.int32)
        h_row = lax.dynamic_slice_in_dim(hidden_states, center, 1, 0)[0]
        v_row = lax.dynamic_slice_in_dim(vals, center, 1, 0)[0]
        i_row = lax.dynamic_slice_in_dim(class_ids, center, 1, 0)[0]
        inner_h = jnp.dot(hidden_states, h_row, preferred_element_type=jnp.float32)

        def block(pair):
            values, idents = pair
            match = idents.reshape(-1, nblk, K_LOC, 1) == i_row.reshape(1, nblk, 1, K_LOC)
            prod = values.reshape(-1, nblk, K_LOC, 1) * v_row.reshape(1, nblk, 1, K_LOC)
            return jnp.sum(jnp.where(match, prod, jnp.float32(0.0)), axis=(1, 2, 3))

        inner_a = lax.map(block, (vals.reshape(groups, SAMP_DEV, TOPK), class_ids.reshape(groups, SAMP_DEV, TOPK))).reshape(POOL)
        norm_hc = jnp.sum(jnp.square(h_row.astype(jnp.float32)))
        norm_ac = jnp.sum(v_row * v_row)
        dist = jnp.maximum(sq_h * sq_a + norm_hc * norm_ac - 2.0 * inner_h * inner_a, jnp.float32(0.0))
        min_distance = dist if step == 0 else jnp.minimum(min_distance, dist)
        means.append(jnp.sum(min_distance) / POOL)
    return min_distance, jnp.stack(means)
```

```python
import functools

import jax
import jax.numpy as jnp
from jax import lax
from jax.experimental import pallas as pl
from jax.experimental.pallas import tpu as pltpu
from jax.sharding import PartitionSpec as P

MESH = pl.DeviceIdType.MESH
STEPS = 3
LANES = 128
TALL = 16
NT = (((1,), (1,)), ((), ()))


def kernel(
    DP, MP,
    c_ref, h_hbm, v_hbm, i_hbm,
    dist_ref, mean_ref,
    h, v, ids, ch_buf, meta_buf, ch_slots, meta_slots, part, part_slots, row_buf, row_slots,
    h_sem, i_sem, v_sem, a_send, a_recv, b_send, b_recv, c_send, c_recv, d_send, d_recv,
):
    groups, tall, width = h.shape
    rows = groups * tall
    tiles, depth, _ = ids.shape
    blk = rows // MP
    my_dp = lax.axis_index("dp")
    my_mp = lax.axis_index("mp")
    me = my_dp * MP + my_mp
    f32 = jnp.float32

    copies = [pltpu.make_async_copy(h_hbm, h, h_sem)]
    for j in range(tiles):
        at = pl.ds(j * LANES, LANES)
        copies.append(pltpu.make_async_copy(i_hbm.at[:, at], ids.at[j], i_sem.at[j]))
        copies.append(pltpu.make_async_copy(v_hbm.at[:, at], v.at[j], v_sem.at[j]))
    for copy in copies:
        copy.start()

    barrier = pltpu.get_barrier_semaphore()
    for d in range(1, DP):
        pl.semaphore_signal(
            barrier, inc=1, device_id=(lax.rem(my_dp + d, DP), my_mp), device_id_type=MESH
        )
    for d in range(1, MP):
        pl.semaphore_signal(
            barrier, inc=1, device_id=(my_dp, lax.rem(my_mp + d, MP)), device_id_type=MESH
        )
    for copy in copies:
        copy.wait()

    lane = lax.broadcasted_iota(jnp.int32, (2 * depth, LANES), 1)
    row16 = lax.broadcasted_iota(jnp.int32, (tall, 1), 0)
    picks = []
    meta = jnp.zeros((2 * depth, LANES), f32)
    for t in range(STEPS):
        c = c_ref[t]
        off = lax.rem(c, rows)
        g = lax.div(off, tall)
        tile = h[g].astype(f32)
        hit = row16 + (my_dp * rows + g * tall) == c
        picks.append(jnp.sum(jnp.where(hit, tile, 0.0), axis=0, keepdims=True))
        g = lax.div(off, LANES)
        both = jnp.concatenate([ids[g].astype(f32), v[g].astype(f32)], axis=0)
        lhit = lane + (my_dp * rows + g * LANES) == c
        col = jnp.sum(jnp.where(lhit, both, 0.0), axis=1, keepdims=True)
        meta = jnp.where(lane == t, col, meta)
    picks.append(jnp.zeros((1, width), f32))
    ch_buf[...] = jnp.concatenate(picks, axis=0).astype(jnp.bfloat16)
    wide = jnp.concatenate([meta, jnp.zeros((LANES - 2 * depth, LANES), f32)], axis=0)
    meta_buf[...] = wide.T[0:8, :]

    pl.semaphore_wait(barrier, DP - 1 + MP - 1)
    sends = []
    for d in range(1, DP):
        to = (lax.rem(my_dp + d, DP), my_mp)
        for src, dst, ss, rs in (
            (ch_buf, ch_slots, a_send, a_recv),
            (meta_buf, meta_slots, b_send, b_recv),
        ):
            copy = pltpu.make_async_remote_copy(
                src_ref=src, dst_ref=dst.at[d - 1],
                send_sem=ss.at[d - 1], recv_sem=rs.at[d - 1],
                device_id=to, device_id_type=MESH,
            )
            copy.start()
            sends.append(copy)

    ones = jnp.ones((8, LANES), jnp.bfloat16)
    for b in range(MP):
        y = jnp.zeros((blk // tall, tall, LANES), f32)
        for j in range(width // LANES):
            x = h[b * blk // tall:(b + 1) * blk // tall, :, j * LANES:(j + 1) * LANES].astype(f32)
            y = y + x * x
        y = y.reshape(blk, LANES)
        hi = y.astype(jnp.bfloat16)
        lo = (y - hi.astype(f32)).astype(jnp.bfloat16)
        sq = lax.dot_general(ones, hi, NT, preferred_element_type=f32)
        sq = sq + lax.dot_general(ones, lo, NT, preferred_element_type=f32)
        part[b, 3:4, 0:blk] = sq[0:1]
        for j in range(blk // LANES):
            a = v[b * blk // LANES + j].astype(f32)
            part[b, 7:8, j * LANES:(j + 1) * LANES] = jnp.sum(a * a, axis=0, keepdims=True)

    for copy in sends:
        copy.wait_recv()
    ch4 = ch_buf[...].astype(f32)
    cm = meta_buf[...]
    for d in range(DP - 1):
        ch4 = ch4 + ch_slots[d].astype(f32)
        cm = cm + meta_slots[d]
    ch = jnp.concatenate([ch4, jnp.zeros_like(ch4)], axis=0).astype(jnp.bfloat16)
    nh = jnp.sum(ch4 * ch4, axis=1, keepdims=True)
    lane8 = lax.broadcasted_iota(jnp.int32, (8, LANES), 1)
    na = jnp.sum(jnp.where(lane8 >= depth, cm * cm, 0.0), axis=1, keepdims=True)
    norms = jnp.broadcast_to(jnp.concatenate([nh, na[0:4]], axis=0), (8, LANES))
    cols = jnp.concatenate([cm, jnp.zeros((LANES - 8, LANES), f32)], axis=0).T
    id_cols = [
        jnp.broadcast_to(cols[0:depth, t:t + 1], (depth, LANES)).astype(jnp.int32)
        for t in range(STEPS)
    ]
    v_cols = [
        jnp.broadcast_to(cols[depth:2 * depth, t:t + 1], (depth, LANES)) for t in range(STEPS)
    ]

    outs = []
    for d in list(range(1, MP)) + [0]:
        b = lax.rem(my_mp + d, MP)
        hb = h[pl.ds(b * (blk // tall), blk // tall)].reshape(blk, width)
        hh = lax.dot_general(ch, hb, NT, preferred_element_type=f32)
        part[b, 0:STEPS, 0:blk] = hh[0:STEPS]
        part[b, :, blk:] = norms
        for j in range(blk // LANES):
            bid = ids[b * (blk // LANES) + j]
            bv = v[b * (blk // LANES) + j].astype(f32)
            for t in range(STEPS):
                w = jnp.zeros((depth, LANES), f32)
                for l in range(depth):
                    w = jnp.where(bid == id_cols[t][l:l + 1], v_cols[t][l:l + 1], w)
                part[b, 4 + t:5 + t, j * LANES:(j + 1) * LANES] = jnp.sum(
                    bv * w, axis=0, keepdims=True
                )
        if d:
            copy = pltpu.make_async_remote_copy(
                src_ref=part.at[b], dst_ref=part_slots.at[d - 1],
                send_sem=c_send.at[d - 1], recv_sem=c_recv.at[d - 1],
                device_id=(my_dp, b), device_id_type=MESH,
            )
            copy.start()
            outs.append(copy)
    total = part[my_mp]
    for d, copy in enumerate(outs):
        copy.wait_recv()
        total = total + part_slots[d]

    pq = total[0:4] * total[4:8]
    lane1 = lax.broadcasted_iota(jnp.int32, (1, LANES), 1)
    own = pq[3:4, 0:blk]
    row = jnp.zeros((1, LANES), f32)
    low = None
    for t in range(STEPS):
        center = jnp.concatenate([pq[t:t + 1, blk:]] * (blk // LANES), axis=1)
        dist = jnp.maximum(own + center - 2.0 * pq[t:t + 1, 0:blk], 0.0)
        low = dist if low is None else jnp.minimum(low, dist)
        row = jnp.where(lane1 == t, jnp.sum(low, axis=1, keepdims=True), row)
    row_buf[...] = row
    lasts = []
    for d in range(1, DP * MP):
        to = lax.rem(me + d, DP * MP)
        copy = pltpu.make_async_remote_copy(
            src_ref=row_buf, dst_ref=row_slots.at[pl.ds(me, 1)],
            send_sem=d_send.at[d - 1], recv_sem=d_recv.at[d - 1],
            device_id=(lax.div(to, MP), lax.rem(to, MP)), device_id_type=MESH,
        )
        copy.start()
        lasts.append(copy)
    row_slots[pl.ds(me, 1), :] = row
    dist_ref[...] = low
    for copy in sends + outs:
        copy.wait_send()
    for copy in lasts:
        copy.wait()
    mean_ref[...] = jnp.sum(row_slots[...], axis=0, keepdims=True) / (blk * MP * DP)


def solution(mesh):
    DP, MP = mesh.shape["dp"], mesh.shape["mp"]

    def body(hidden_states, factor_values, class_ids, centers):
        rows, width = hidden_states.shape
        depth = class_ids.shape[1]
        blk = rows // MP
        vm = pltpu.VMEM
        sem = pltpu.SemaphoreType.DMA
        hbm = pl.BlockSpec(memory_space=pl.ANY)
        low, mean = pl.pallas_call(
            functools.partial(kernel, DP, MP),
            out_shape=(
                jax.ShapeDtypeStruct((1, blk), jnp.float32),
                jax.ShapeDtypeStruct((1, LANES), jnp.float32),
            ),
            in_specs=[pl.BlockSpec(memory_space=pltpu.SMEM), hbm, hbm, hbm],
            out_specs=(pl.BlockSpec(memory_space=vm), pl.BlockSpec(memory_space=vm)),
            scratch_shapes=[
                vm((rows // TALL, TALL, width), jnp.bfloat16),
                vm((rows // LANES, depth, LANES), jnp.bfloat16),
                vm((rows // LANES, depth, LANES), jnp.int32),
                vm((4, width), jnp.bfloat16),
                vm((8, LANES), jnp.float32),
                vm((DP - 1, 4, width), jnp.bfloat16),
                vm((DP - 1, 8, LANES), jnp.float32),
                vm((MP, 8, blk + LANES), jnp.float32),
                vm((MP - 1, 8, blk + LANES), jnp.float32),
                vm((1, LANES), jnp.float32),
                vm((DP * MP, LANES), jnp.float32),
                sem, sem((rows // LANES,)), sem((rows // LANES,)),
                sem((DP - 1,)), sem((DP - 1,)), sem((DP - 1,)), sem((DP - 1,)),
                sem((MP - 1,)), sem((MP - 1,)),
                sem((DP * MP - 1,)), sem((DP * MP - 1,)),
            ],
            compiler_params=pltpu.CompilerParams(collective_id=0, has_side_effects=True),
        )(centers, hidden_states.reshape(rows // TALL, TALL, width), factor_values.T, class_ids.T)
        return low.reshape(blk), mean[0, :STEPS]

    return jax.shard_map(
        body,
        mesh=mesh,
        in_specs=(P("dp", "mp"), P("dp", "mp"), P("dp", "mp"), P()),
        out_specs=(P(("dp", "mp")), P()),
        check_vma=False,
    )
```

```python
import functools

import jax
import jax.numpy as jnp
from jax import lax
from jax.experimental import pallas as pl
from jax.experimental.pallas import tpu as pltpu
from jax.sharding import PartitionSpec as P

MESH = pl.DeviceIdType.MESH
STEPS = 3
LANES = 128
TALL = 16
NT = (((1,), (1,)), ((), ()))


def partner(p, k, n):
    if n & (n - 1):
        return lax.rem(p + k, n)
    bit = 1
    q = p
    while bit <= k:
        if k & bit:
            q = q + bit - 2 * bit * lax.rem(lax.div(p, bit), 2)
        bit *= 2
    return q


def kernel(
    DP, MP,
    c_hbm, h_hbm, v_hbm, i_hbm,
    dist_ref, mean_ref,
    c_ref, h, v, ids, ch_buf, ch_slots, sq, sq_slots, norm_buf, norm_slots, part, part_slots,
    row_buf, row_slots,
    z_sem, h_sem, i_sem, v_sem, a_send, a_recv, s_send, s_recv, n_send, n_recv, b_send, b_recv,
    d_send, d_recv,
):
    groups, tall, width = h.shape
    rows = groups * tall
    tiles, depth, _ = ids.shape
    blk = rows // MP
    my_dp = lax.axis_index("dp")
    my_mp = lax.axis_index("mp")
    me = my_dp * MP + my_mp
    f32 = jnp.float32

    copies = [
        pltpu.make_async_copy(c_hbm, c_ref, z_sem), pltpu.make_async_copy(h_hbm, h, h_sem)
    ]
    for j in range(tiles):
        at = pl.ds(j * LANES, LANES)
        copies.append(pltpu.make_async_copy(i_hbm.at[:, at], ids.at[j], i_sem.at[j]))
        copies.append(pltpu.make_async_copy(v_hbm.at[:, at], v.at[j], v_sem.at[j]))
    for copy in copies:
        copy.start()

    barrier = pltpu.get_barrier_semaphore()
    for d in range(1, DP):
        pl.semaphore_signal(
            barrier, inc=1, device_id=(lax.rem(my_dp + d, DP), my_mp), device_id_type=MESH
        )
    for d in range(1, MP):
        pl.semaphore_signal(
            barrier, inc=1, device_id=(my_dp, lax.rem(my_mp + d, MP)), device_id_type=MESH
        )
    for copy in copies:
        copy.wait()

    lane = lax.broadcasted_iota(jnp.int32, (4 * depth, LANES), 1)
    row16 = lax.broadcasted_iota(jnp.int32, (tall, 1), 0)
    picks = []
    meta = jnp.zeros((4 * depth, LANES), f32)
    for t in range(STEPS):
        c = c_ref[t]
        off = lax.rem(c, rows)
        g = lax.div(off, tall)
        tile = h[g].astype(f32)
        hit = row16 + (my_dp * rows + g * tall) == c
        picks.append(jnp.sum(jnp.where(hit, tile, 0.0), axis=0, keepdims=True))
        g = lax.div(off, LANES)
        k = ids[g]
        digits = [(k >> 12).astype(f32), ((k >> 6) & 63).astype(f32), (k & 63).astype(f32)]
        both = jnp.concatenate(digits + [v[g].astype(f32)], axis=0)
        lhit = lane + (my_dp * rows + g * LANES) == c
        col = jnp.sum(jnp.where(lhit, both, 0.0), axis=1, keepdims=True)
        meta = jnp.where(lane == t, col, meta)
    wide = jnp.concatenate([meta, jnp.zeros((LANES - 4 * depth, LANES), f32)], axis=0).T
    tail = [wide[t:t + 1] for t in range(STEPS)] + [jnp.zeros((1, width - STEPS * LANES), f32)]
    picks.append(jnp.concatenate(tail, axis=1))
    ch_buf[...] = jnp.concatenate(picks, axis=0).astype(jnp.bfloat16)

    pl.semaphore_wait(barrier, DP - 1 + MP - 1)
    sends = []
    for d in range(1, DP):
        copy = pltpu.make_async_remote_copy(
            src_ref=ch_buf, dst_ref=ch_slots.at[d - 1],
            send_sem=a_send.at[d - 1], recv_sem=a_recv.at[d - 1],
            device_id=(lax.rem(my_dp + d, DP), my_mp), device_id_type=MESH,
        )
        copy.start()
        sends.append(copy)

    ones = jnp.ones((8, LANES), jnp.bfloat16)
    for b in range(MP):
        y = jnp.zeros((blk // tall, tall, LANES), f32)
        for j in range(width // LANES):
            x = h[b * blk // tall:(b + 1) * blk // tall, :, j * LANES:(j + 1) * LANES].astype(f32)
            y = y + x * x
        y = y.reshape(blk, LANES)
        hi = y.astype(jnp.bfloat16)
        lo = (y - hi.astype(f32)).astype(jnp.bfloat16)
        norm = lax.dot_general(ones, hi, NT, preferred_element_type=f32)
        norm = norm + lax.dot_general(ones, lo, NT, preferred_element_type=f32)
        sq[b, 0:1] = norm[0:1]
        for j in range(blk // LANES):
            a = v[b * blk // LANES + j].astype(f32)
            sq[b, 1:2, j * LANES:(j + 1) * LANES] = jnp.sum(a * a, axis=0, keepdims=True)
    order = [(k, partner(my_mp, k, MP)) for k in reversed(range(1, MP))]
    early = []
    for k, b in order:
        copy = pltpu.make_async_remote_copy(
            src_ref=sq.at[b], dst_ref=sq_slots.at[k - 1],
            send_sem=s_send.at[k - 1], recv_sem=s_recv.at[k - 1],
            device_id=(my_dp, b), device_id_type=MESH,
        )
        copy.start()
        early.append(copy)

    for copy in sends:
        copy.wait_recv()
    ch4 = ch_buf[...].astype(f32)
    for d in range(DP - 1):
        ch4 = ch4 + ch_slots[d].astype(f32)
    ch = jnp.concatenate([ch4, jnp.zeros_like(ch4)], axis=0).astype(jnp.bfloat16)
    cm = jnp.concatenate(
        [ch4[3:4, t * LANES:(t + 1) * LANES] for t in range(STEPS)]
        + [jnp.zeros((LANES - STEPS, LANES), f32)],
        axis=0,
    )
    nh = jnp.sum(ch4 * ch4, axis=1, keepdims=True)
    lane8 = lax.broadcasted_iota(jnp.int32, (8, LANES), 1)
    cm8 = jnp.where(lane8 >= 3 * depth, cm[0:8], 0.0)
    na = jnp.sum(cm8 * cm8, axis=1, keepdims=True)
    lane1 = lax.broadcasted_iota(jnp.int32, (1, LANES), 1)
    norms = jnp.zeros((1, LANES), f32)
    for t in range(STEPS):
        norms = jnp.where(lane1 == t, nh[t:t + 1], norms)
        norms = jnp.where(lane1 == STEPS + t, na[t:t + 1], norms)
    norm_buf[...] = norms
    for k, b in order:
        copy = pltpu.make_async_remote_copy(
            src_ref=norm_buf, dst_ref=norm_slots.at[k - 1],
            send_sem=n_send.at[k - 1], recv_sem=n_recv.at[k - 1],
            device_id=(my_dp, b), device_id_type=MESH,
        )
        copy.start()
        early.append(copy)
    cols = cm.T
    id_cols, v_cols = [], []
    for t in range(STEPS):
        col = jnp.broadcast_to(cols[0:4 * depth, t:t + 1], (4 * depth, LANES))
        code = col[0:depth] * 4096.0 + col[depth:2 * depth] * 64.0 + col[2 * depth:3 * depth]
        id_cols.append(code.astype(jnp.int32))
        v_cols.append(col[3 * depth:])

    outs = []
    for d, b in order + [(0, my_mp)]:
        hb = h[pl.ds(b * (blk // tall), blk // tall)].reshape(blk, width)
        hh = lax.dot_general(ch, hb, NT, preferred_element_type=f32)
        part[b, 0:STEPS] = hh[0:STEPS]
        for j in range(blk // LANES):
            bid = ids[b * (blk // LANES) + j]
            bv = v[b * (blk // LANES) + j].astype(f32)
            for t in range(STEPS):
                w = jnp.zeros((depth, LANES), f32)
                for l in range(depth):
                    w = jnp.where(bid == id_cols[t][l:l + 1], v_cols[t][l:l + 1], w)
                part[b, STEPS + t:STEPS + t + 1, j * LANES:(j + 1) * LANES] = jnp.sum(
                    bv * w, axis=0, keepdims=True
                )
        if d:
            copy = pltpu.make_async_remote_copy(
                src_ref=part.at[b], dst_ref=part_slots.at[d - 1],
                send_sem=b_send.at[d - 1], recv_sem=b_recv.at[d - 1],
                device_id=(my_dp, b), device_id_type=MESH,
            )
            copy.start()
            outs.append(copy)
    own, norms, total = sq[my_mp], norm_buf[...], part[my_mp]
    for copy in early + outs:
        copy.wait_recv()
    for k in range(MP - 1):
        own = own + sq_slots[k]
        norms = norms + norm_slots[k]
        total = total + part_slots[k]

    own = own[0:1] * own[1:2]
    row = jnp.zeros((1, LANES), f32)
    low = None
    for t in range(STEPS):
        center = norms[:, t:t + 1] * norms[:, STEPS + t:STEPS + t + 1]
        cross = total[t:t + 1] * total[STEPS + t:STEPS + t + 1]
        dist = jnp.maximum(own + center - 2.0 * cross, 0.0)
        low = dist if low is None else jnp.minimum(low, dist)
        row = jnp.where(lane1 == t, jnp.sum(low, axis=1, keepdims=True), row)
    row_buf[...] = row
    lasts = []
    for d in range(1, DP * MP):
        to = lax.rem(me + d, DP * MP)
        copy = pltpu.make_async_remote_copy(
            src_ref=row_buf, dst_ref=row_slots.at[pl.ds(me, 1)],
            send_sem=d_send.at[d - 1], recv_sem=d_recv.at[d - 1],
            device_id=(lax.div(to, MP), lax.rem(to, MP)), device_id_type=MESH,
        )
        copy.start()
        lasts.append(copy)
    row_slots[pl.ds(me, 1), :] = row
    dist_ref[...] = low
    for copy in sends + early + outs:
        copy.wait_send()
    for copy in lasts:
        copy.wait()
    mean_ref[...] = jnp.sum(row_slots[...], axis=0, keepdims=True) / (blk * MP * DP)


def solution(mesh):
    DP, MP = mesh.shape["dp"], mesh.shape["mp"]

    def body(hidden_states, factor_values, class_ids, centers):
        rows, width = hidden_states.shape
        depth = class_ids.shape[1]
        blk = rows // MP
        vm = pltpu.VMEM
        sem = pltpu.SemaphoreType.DMA
        hbm = pl.BlockSpec(memory_space=pl.ANY)
        low, mean = pl.pallas_call(
            functools.partial(kernel, DP, MP),
            out_shape=(vm((1, blk), jnp.float32), vm((1, LANES), jnp.float32)),
            in_specs=[hbm] * 4,
            out_specs=(pl.BlockSpec(memory_space=vm), pl.BlockSpec(memory_space=vm)),
            scratch_shapes=[
                pltpu.SMEM((STEPS,), jnp.int32),
                vm((rows // TALL, TALL, width), jnp.bfloat16),
                vm((rows // LANES, depth, LANES), jnp.bfloat16),
                vm((rows // LANES, depth, LANES), jnp.int32),
                vm((4, width), jnp.bfloat16),
                vm((DP - 1, 4, width), jnp.bfloat16),
                vm((MP, 2, blk), jnp.float32),
                vm((MP - 1, 2, blk), jnp.float32),
                vm((1, LANES), jnp.float32),
                vm((MP - 1, 1, LANES), jnp.float32),
                vm((MP, 2 * STEPS, blk), jnp.float32),
                vm((MP - 1, 2 * STEPS, blk), jnp.float32),
                vm((1, LANES), jnp.float32),
                vm((DP * MP, LANES), jnp.float32),
                sem, sem, sem((rows // LANES,)), sem((rows // LANES,)),
                sem((DP - 1,)), sem((DP - 1,)),
                sem((MP - 1,)), sem((MP - 1,)),
                sem((MP - 1,)), sem((MP - 1,)),
                sem((MP - 1,)), sem((MP - 1,)),
                sem((DP * MP - 1,)), sem((DP * MP - 1,)),
            ],
            compiler_params=pltpu.CompilerParams(collective_id=0, has_side_effects=True),
        )(centers, hidden_states.reshape(rows // TALL, TALL, width), factor_values.T, class_ids.T)
        return low.reshape(blk), mean[0, :STEPS]

    return jax.shard_map(
        body,
        mesh=mesh,
        in_specs=(P("dp", "mp"), P("dp", "mp"), P("dp", "mp"), P()),
        out_specs=(P(("dp", "mp")), P()),
        check_vma=False,
    )
```

```python
import functools

import jax
import jax.numpy as jnp
from jax import lax
from jax.experimental import pallas as pl
from jax.experimental.pallas import tpu as pltpu
from jax.sharding import PartitionSpec as P

MESH = pl.DeviceIdType.MESH
STEPS = 3
LANES = 128
TALL = 16
CHUNKS = 8
NT = (((1,), (1,)), ((), ()))


def partner(p, k, n):
    if n & (n - 1):
        return lax.rem(p + k, n)
    bit = 1
    q = p
    while bit <= k:
        if k & bit:
            q = q + bit - 2 * bit * lax.rem(lax.div(p, bit), 2)
        bit *= 2
    return q


def drain(ref, sem):
    pltpu.make_async_copy(ref, ref, sem).wait()


def kernel(
    DP, MP,
    c_hbm, h_hbm, v_hbm, i_hbm,
    dist_ref, mean_ref,
    c_ref, h, v, ids, ch_buf, ch_slots, sq, sq_slots, norm_buf, norm_slots, part, part_slots,
    row_buf, row_slots,
    z_sem, h_sem, i_sem, v_sem, a_send, a_recv, s_send, s_recv, n_send, n_recv, b_send, b_recv,
    d_send, d_recv,
):
    groups, tall, width = h.shape
    rows = groups * tall
    tiles, depth, _ = ids.shape
    blk = rows // MP
    my_dp = lax.axis_index("dp")
    my_mp = lax.axis_index("mp")
    me = my_dp * MP + my_mp
    f32 = jnp.float32
    dp_peers = [partner(my_dp, k, DP) for k in range(DP)]
    mp_peers = [partner(my_mp, k, MP) for k in range(MP)]

    pltpu.make_async_copy(c_hbm, c_ref, z_sem).start()
    step = max(groups // CHUNKS, 1)
    for j in range(0, groups, step):
        at = pl.ds(j, step)
        pltpu.make_async_copy(h_hbm.at[at], h.at[at], h_sem).start()
    for j in range(tiles):
        at = pl.ds(j * LANES, LANES)
        pltpu.make_async_copy(i_hbm.at[:, at], ids.at[j], i_sem).start()
        pltpu.make_async_copy(v_hbm.at[:, at], v.at[j], v_sem).start()

    barrier = pltpu.get_barrier_semaphore()
    for d in range(1, DP):
        pl.semaphore_signal(
            barrier, inc=1, device_id=(lax.rem(my_dp + d, DP), my_mp), device_id_type=MESH
        )
    for d in range(1, MP):
        pl.semaphore_signal(
            barrier, inc=1, device_id=(my_dp, lax.rem(my_mp + d, MP)), device_id_type=MESH
        )
    pltpu.make_async_copy(c_hbm, c_ref, z_sem).wait()
    drain(ids, i_sem)
    drain(v, v_sem)

    lane = lax.broadcasted_iota(jnp.int32, (4 * depth, LANES), 1)
    row16 = lax.broadcasted_iota(jnp.int32, (tall, 1), 0)
    first = my_dp * rows
    offs = [lax.rem(c_ref[t], rows) for t in range(STEPS)]
    meta = jnp.zeros((4 * depth, LANES), f32)
    for t in range(STEPS):
        g = lax.div(offs[t], LANES)
        k = ids[g]
        digits = [(k >> 12).astype(f32), ((k >> 6) & 63).astype(f32), (k & 63).astype(f32)]
        both = jnp.concatenate(digits + [v[g].astype(f32)], axis=0)
        hit = lane + (first + g * LANES) == c_ref[t]
        col = jnp.sum(jnp.where(hit, both, 0.0), axis=1, keepdims=True)
        meta = jnp.where(lane == t, col, meta)
    wide = jnp.concatenate([meta, jnp.zeros((LANES - 4 * depth, LANES), f32)], axis=0).T
    drain(h, h_sem)
    picks = []
    for t in range(STEPS):
        g = lax.div(offs[t], tall)
        hit = row16 + (first + g * tall) == c_ref[t]
        picks.append(jnp.sum(jnp.where(hit, h[g].astype(f32), 0.0), axis=0, keepdims=True))
    tail = [wide[t:t + 1] for t in range(STEPS)] + [jnp.zeros((1, width - STEPS * LANES), f32)]
    picks.append(jnp.concatenate(tail, axis=1))
    ch_buf[...] = jnp.concatenate(picks, axis=0).astype(jnp.bfloat16)

    pl.semaphore_wait(barrier, DP - 1 + MP - 1)
    for k in reversed(range(1, DP)):
        pltpu.make_async_remote_copy(
            src_ref=ch_buf, dst_ref=ch_slots.at[k - 1], send_sem=a_send, recv_sem=a_recv,
            device_id=(dp_peers[k], my_mp), device_id_type=MESH,
        ).start()

    ones = jnp.ones((8, LANES), jnp.bfloat16)
    for b in range(MP):
        y = jnp.zeros((blk // tall, tall, LANES), f32)
        for j in range(width // LANES):
            x = h[b * blk // tall:(b + 1) * blk // tall, :, j * LANES:(j + 1) * LANES].astype(f32)
            y = y + x * x
        y = y.reshape(blk, LANES)
        hi = y.astype(jnp.bfloat16)
        lo = (y - hi.astype(f32)).astype(jnp.bfloat16)
        norm = lax.dot_general(ones, hi, NT, preferred_element_type=f32)
        norm = norm + lax.dot_general(ones, lo, NT, preferred_element_type=f32)
        sq[b, 0:1] = norm[0:1]
        for j in range(blk // LANES):
            a = v[b * blk // LANES + j].astype(f32)
            sq[b, 1:2, j * LANES:(j + 1) * LANES] = jnp.sum(a * a, axis=0, keepdims=True)
    for k in reversed(range(1, MP)):
        pltpu.make_async_remote_copy(
            src_ref=sq.at[mp_peers[k]], dst_ref=sq_slots.at[k - 1], send_sem=s_send, recv_sem=s_recv,
            device_id=(my_dp, mp_peers[k]), device_id_type=MESH,
        ).start()

    drain(ch_slots, a_recv)
    ch4 = ch_buf[...].astype(f32)
    for d in range(DP - 1):
        ch4 = ch4 + ch_slots[d].astype(f32)
    ch = jnp.concatenate([ch4, jnp.zeros_like(ch4)], axis=0).astype(jnp.bfloat16)
    cm = jnp.concatenate(
        [ch4[3:4, t * LANES:(t + 1) * LANES] for t in range(STEPS)]
        + [jnp.zeros((LANES - STEPS, LANES), f32)],
        axis=0,
    )
    nh = jnp.sum(ch4 * ch4, axis=1, keepdims=True)
    lane8 = lax.broadcasted_iota(jnp.int32, (8, LANES), 1)
    cm8 = jnp.where(lane8 >= 3 * depth, cm[0:8], 0.0)
    na = jnp.sum(cm8 * cm8, axis=1, keepdims=True)
    lane1 = lax.broadcasted_iota(jnp.int32, (1, LANES), 1)
    norms = jnp.zeros((1, LANES), f32)
    for t in range(STEPS):
        norms = jnp.where(lane1 == t, nh[t:t + 1], norms)
        norms = jnp.where(lane1 == STEPS + t, na[t:t + 1], norms)
    norm_buf[...] = norms
    for k in reversed(range(1, MP)):
        pltpu.make_async_remote_copy(
            src_ref=norm_buf, dst_ref=norm_slots.at[k - 1], send_sem=n_send, recv_sem=n_recv,
            device_id=(my_dp, mp_peers[k]), device_id_type=MESH,
        ).start()
    cols = cm.T
    id_cols, v_cols = [], []
    for t in range(STEPS):
        col = jnp.broadcast_to(cols[0:4 * depth, t:t + 1], (4 * depth, LANES))
        code = col[0:depth] * 4096.0 + col[depth:2 * depth] * 64.0 + col[2 * depth:3 * depth]
        id_cols.append(code.astype(jnp.int32))
        v_cols.append(col[3 * depth:])

    for k in reversed(range(MP)):
        b = mp_peers[k]
        hb = h[pl.ds(b * (blk // tall), blk // tall)].reshape(blk, width)
        hh = lax.dot_general(ch, hb, NT, preferred_element_type=f32)
        part[b, 0:STEPS] = hh[0:STEPS]
        for j in range(blk // LANES):
            bid = ids[b * (blk // LANES) + j]
            bv = v[b * (blk // LANES) + j].astype(f32)
            for t in range(STEPS):
                w = jnp.zeros((depth, LANES), f32)
                for l in range(depth):
                    w = jnp.where(bid == id_cols[t][l:l + 1], v_cols[t][l:l + 1], w)
                part[b, STEPS + t:STEPS + t + 1, j * LANES:(j + 1) * LANES] = jnp.sum(
                    bv * w, axis=0, keepdims=True
                )
        if k:
            pltpu.make_async_remote_copy(
                src_ref=part.at[b], dst_ref=part_slots.at[k - 1], send_sem=b_send, recv_sem=b_recv,
                device_id=(my_dp, b), device_id_type=MESH,
            ).start()
    own, norms = sq[my_mp], norm_buf[...]
    drain(sq_slots, s_recv)
    drain(norm_slots, n_recv)
    for k in range(MP - 1):
        own = own + sq_slots[k]
        norms = norms + norm_slots[k]
    own = own[0:1] * own[1:2]
    bases = [own + norms[:, t:t + 1] * norms[:, STEPS + t:STEPS + t + 1] for t in range(STEPS)]
    total = part[my_mp]
    drain(part_slots, b_recv)
    for k in range(MP - 1):
        total = total + part_slots[k]
    row = jnp.zeros((1, LANES), f32)
    low = None
    for t in range(STEPS):
        cross = total[t:t + 1] * total[STEPS + t:STEPS + t + 1]
        dist = jnp.maximum(bases[t] - 2.0 * cross, 0.0)
        low = dist if low is None else jnp.minimum(low, dist)
        row = jnp.where(lane1 == t, jnp.sum(low, axis=1, keepdims=True), row)
    row_buf[...] = row
    for kd in reversed(range(DP)):
        for km in reversed(range(MP)):
            if kd or km:
                pltpu.make_async_remote_copy(
                    src_ref=row_buf, dst_ref=row_slots.at[pl.ds(me, 1)],
                    send_sem=d_send, recv_sem=d_recv,
                    device_id=(dp_peers[kd], mp_peers[km]), device_id_type=MESH,
                ).start()
    row_slots[pl.ds(me, 1), :] = row
    dist_ref[...] = low
    drain(ch_slots, a_send)
    drain(sq_slots, s_send)
    drain(norm_slots, n_send)
    drain(part_slots, b_send)
    others = row_slots.at[pl.ds(0, DP * MP - 1)]
    drain(others, d_send)
    drain(others, d_recv)
    mean_ref[...] = jnp.sum(row_slots[...], axis=0, keepdims=True) / (blk * MP * DP)


def solution(mesh):
    DP, MP = mesh.shape["dp"], mesh.shape["mp"]

    def body(hidden_states, factor_values, class_ids, centers):
        rows, width = hidden_states.shape
        depth = class_ids.shape[1]
        blk = rows // MP
        vm = pltpu.VMEM
        sem = pltpu.SemaphoreType.DMA
        hbm = pl.BlockSpec(memory_space=pl.ANY)
        low, mean = pl.pallas_call(
            functools.partial(kernel, DP, MP),
            out_shape=(vm((1, blk), jnp.float32), vm((1, LANES), jnp.float32)),
            in_specs=[hbm] * 4,
            out_specs=(pl.BlockSpec(memory_space=vm), pl.BlockSpec(memory_space=vm)),
            scratch_shapes=[
                pltpu.SMEM((STEPS,), jnp.int32),
                vm((rows // TALL, TALL, width), jnp.bfloat16),
                vm((rows // LANES, depth, LANES), jnp.bfloat16),
                vm((rows // LANES, depth, LANES), jnp.int32),
                vm((4, width), jnp.bfloat16),
                vm((DP - 1, 4, width), jnp.bfloat16),
                vm((MP, 2, blk), jnp.float32),
                vm((MP - 1, 2, blk), jnp.float32),
                vm((1, LANES), jnp.float32),
                vm((MP - 1, 1, LANES), jnp.float32),
                vm((MP, 2 * STEPS, blk), jnp.float32),
                vm((MP - 1, 2 * STEPS, blk), jnp.float32),
                vm((1, LANES), jnp.float32),
                vm((DP * MP, LANES), jnp.float32),
                *[sem] * 14,
            ],
            compiler_params=pltpu.CompilerParams(collective_id=0, has_side_effects=True),
        )(centers, hidden_states.reshape(rows // TALL, TALL, width), factor_values.T, class_ids.T)
        return low.reshape(blk), mean[0, :STEPS]

    return jax.shard_map(
        body,
        mesh=mesh,
        in_specs=(P("dp", "mp"), P("dp", "mp"), P("dp", "mp"), P()),
        out_specs=(P(("dp", "mp")), P()),
        check_vma=False,
    )
```

```python
import functools

import jax
import jax.numpy as jnp
from jax import lax
from jax.experimental import pallas as pl
from jax.experimental.pallas import tpu as pltpu
from jax.sharding import PartitionSpec as P

MESH = pl.DeviceIdType.MESH
STEPS = 3
LANES = 128
TALL = 16
CHUNKS = 8
NT = (((1,), (1,)), ((), ()))


def partner(p, k, n):
    if n & (n - 1):
        return lax.rem(p + k, n)
    bit = 1
    q = p
    while bit <= k:
        if k & bit:
            q = q + bit - 2 * bit * lax.rem(lax.div(p, bit), 2)
        bit *= 2
    return q


def drain(ref, sem):
    pltpu.make_async_copy(ref, ref, sem).wait()


def finish(low_ref, mean_ref, dist_ref, means_ref):
    dist_ref[...] = low_ref[...]
    means_ref[...] = mean_ref[0:STEPS]


def kernel(
    DP, MP,
    c_hbm, h_hbm, v_hbm, i_hbm,
    dist_ref, mean_ref,
    c_ref, h, v, ids, ch_buf, ch_slots, sq, sq_slots, norm_buf, norm_slots, part, part_slots,
    row_buf, row_slots,
    z_sem, h_sem, i_sem, v_sem, a_send, a_recv, s_send, s_recv, n_send, n_recv, b_send, b_recv,
    d_send, d_recv,
):
    groups, tall, width = h.shape
    rows = groups * tall
    tiles, depth, _ = ids.shape
    blk = rows // MP
    my_dp = lax.axis_index("dp")
    my_mp = lax.axis_index("mp")
    me = my_dp * MP + my_mp
    f32 = jnp.float32
    dp_peers = [partner(my_dp, k, DP) for k in range(DP)]
    mp_peers = [partner(my_mp, k, MP) for k in range(MP)]

    pltpu.make_async_copy(c_hbm, c_ref, z_sem).start()
    step = max(groups // CHUNKS, 1)
    for j in range(0, groups, step):
        at = pl.ds(j, step)
        pltpu.make_async_copy(h_hbm.at[at], h.at[at], h_sem).start()
    for j in range(tiles):
        at = pl.ds(j * LANES, LANES)
        pltpu.make_async_copy(i_hbm.at[:, at], ids.at[j], i_sem).start()
        pltpu.make_async_copy(v_hbm.at[:, at], v.at[j], v_sem).start()

    barrier = pltpu.get_barrier_semaphore()
    for d in range(1, DP):
        pl.semaphore_signal(
            barrier, inc=1, device_id=(lax.rem(my_dp + d, DP), my_mp), device_id_type=MESH
        )
    for d in range(1, MP):
        pl.semaphore_signal(
            barrier, inc=1, device_id=(my_dp, lax.rem(my_mp + d, MP)), device_id_type=MESH
        )
    pltpu.make_async_copy(c_hbm, c_ref, z_sem).wait()
    drain(ids, i_sem)
    drain(v, v_sem)

    lane = lax.broadcasted_iota(jnp.int32, (4 * depth, LANES), 1)
    row16 = lax.broadcasted_iota(jnp.int32, (tall, 1), 0)
    first = my_dp * rows
    offs = [lax.rem(c_ref[t], rows) for t in range(STEPS)]
    meta = jnp.zeros((4 * depth, LANES), f32)
    for t in range(STEPS):
        g = lax.div(offs[t], LANES)
        k = ids[g]
        digits = [(k >> 12).astype(f32), ((k >> 6) & 63).astype(f32), (k & 63).astype(f32)]
        both = jnp.concatenate(digits + [v[g].astype(f32)], axis=0)
        hit = lane + (first + g * LANES) == c_ref[t]
        col = jnp.sum(jnp.where(hit, both, 0.0), axis=1, keepdims=True)
        meta = jnp.where(lane == t, col, meta)
    wide = jnp.concatenate([meta, jnp.zeros((LANES - 4 * depth, LANES), f32)], axis=0).T
    drain(h, h_sem)
    picks = []
    for t in range(STEPS):
        g = lax.div(offs[t], tall)
        hit = row16 + (first + g * tall) == c_ref[t]
        picks.append(jnp.sum(jnp.where(hit, h[g].astype(f32), 0.0), axis=0, keepdims=True))
    tail = [wide[t:t + 1] for t in range(STEPS)] + [jnp.zeros((1, width - STEPS * LANES), f32)]
    picks.append(jnp.concatenate(tail, axis=1))
    ch_buf[...] = jnp.concatenate(picks, axis=0).astype(jnp.bfloat16)

    pl.semaphore_wait(barrier, DP - 1 + MP - 1)
    for k in reversed(range(1, DP)):
        pltpu.make_async_remote_copy(
            src_ref=ch_buf, dst_ref=ch_slots.at[k - 1], send_sem=a_send, recv_sem=a_recv,
            device_id=(dp_peers[k], my_mp), device_id_type=MESH,
        ).start()

    ones = jnp.ones((8, LANES), jnp.bfloat16)
    for b in range(MP):
        y = jnp.zeros((blk // tall, tall, LANES), f32)
        for j in range(width // LANES):
            x = h[b * blk // tall:(b + 1) * blk // tall, :, j * LANES:(j + 1) * LANES].astype(f32)
            y = y + x * x
        y = y.reshape(blk, LANES)
        hi = y.astype(jnp.bfloat16)
        lo = (y - hi.astype(f32)).astype(jnp.bfloat16)
        norm = lax.dot_general(ones, hi, NT, preferred_element_type=f32)
        norm = norm + lax.dot_general(ones, lo, NT, preferred_element_type=f32)
        sq[b, 0:1] = norm[0:1]
        for j in range(blk // LANES):
            a = v[b * blk // LANES + j].astype(f32)
            sq[b, 1:2, j * LANES:(j + 1) * LANES] = jnp.sum(a * a, axis=0, keepdims=True)
    for k in reversed(range(1, MP)):
        pltpu.make_async_remote_copy(
            src_ref=sq.at[mp_peers[k]], dst_ref=sq_slots.at[k - 1], send_sem=s_send, recv_sem=s_recv,
            device_id=(my_dp, mp_peers[k]), device_id_type=MESH,
        ).start()

    drain(ch_slots, a_recv)
    ch4 = ch_buf[...].astype(f32)
    for d in range(DP - 1):
        ch4 = ch4 + ch_slots[d].astype(f32)
    ch = jnp.concatenate([ch4, jnp.zeros_like(ch4)], axis=0).astype(jnp.bfloat16)
    cm = jnp.concatenate(
        [ch4[3:4, t * LANES:(t + 1) * LANES] for t in range(STEPS)]
        + [jnp.zeros((LANES - STEPS, LANES), f32)],
        axis=0,
    )
    nh = jnp.sum(ch4 * ch4, axis=1, keepdims=True)
    lane8 = lax.broadcasted_iota(jnp.int32, (8, LANES), 1)
    cm8 = jnp.where(lane8 >= 3 * depth, cm[0:8], 0.0)
    na = jnp.sum(cm8 * cm8, axis=1, keepdims=True)
    lane1 = lax.broadcasted_iota(jnp.int32, (1, LANES), 1)
    norms = jnp.zeros((1, LANES), f32)
    for t in range(STEPS):
        norms = jnp.where(lane1 == t, nh[t:t + 1], norms)
        norms = jnp.where(lane1 == STEPS + t, na[t:t + 1], norms)
    norm_buf[...] = norms
    for k in reversed(range(1, MP)):
        pltpu.make_async_remote_copy(
            src_ref=norm_buf, dst_ref=norm_slots.at[k - 1], send_sem=n_send, recv_sem=n_recv,
            device_id=(my_dp, mp_peers[k]), device_id_type=MESH,
        ).start()
    cols = cm.T
    id_cols, v_cols = [], []
    for t in range(STEPS):
        col = jnp.broadcast_to(cols[0:4 * depth, t:t + 1], (4 * depth, LANES))
        code = col[0:depth] * 4096.0 + col[depth:2 * depth] * 64.0 + col[2 * depth:3 * depth]
        id_cols.append(code.astype(jnp.int32))
        v_cols.append(col[3 * depth:])

    for k in reversed(range(MP)):
        b = mp_peers[k]
        hb = h[pl.ds(b * (blk // tall), blk // tall)].reshape(blk, width)
        hh = lax.dot_general(ch, hb, NT, preferred_element_type=f32)
        part[b, 0:STEPS] = hh[0:STEPS]
        for j in range(blk // LANES):
            bid = ids[b * (blk // LANES) + j]
            bv = v[b * (blk // LANES) + j].astype(f32)
            for t in range(STEPS):
                w = jnp.zeros((depth, LANES), f32)
                for l in range(depth):
                    w = jnp.where(bid == id_cols[t][l:l + 1], v_cols[t][l:l + 1], w)
                part[b, STEPS + t:STEPS + t + 1, j * LANES:(j + 1) * LANES] = jnp.sum(
                    bv * w, axis=0, keepdims=True
                )
        if k:
            pltpu.make_async_remote_copy(
                src_ref=part.at[b], dst_ref=part_slots.at[k - 1], send_sem=b_send, recv_sem=b_recv,
                device_id=(my_dp, b), device_id_type=MESH,
            ).start()
    own, norms = sq[my_mp], norm_buf[...]
    drain(sq_slots, s_recv)
    drain(norm_slots, n_recv)
    for k in range(MP - 1):
        own = own + sq_slots[k]
        norms = norms + norm_slots[k]
    own = own[0:1] * own[1:2]
    bases = [own + norms[:, t:t + 1] * norms[:, STEPS + t:STEPS + t + 1] for t in range(STEPS)]
    total = part[my_mp]
    drain(part_slots, b_recv)
    for k in range(MP - 1):
        total = total + part_slots[k]
    row = jnp.zeros((1, LANES), f32)
    low = None
    for t in range(STEPS):
        cross = total[t:t + 1] * total[STEPS + t:STEPS + t + 1]
        dist = jnp.maximum(bases[t] - 2.0 * cross, 0.0)
        low = dist if low is None else jnp.minimum(low, dist)
        row = jnp.where(lane1 == t, jnp.sum(low, axis=1, keepdims=True), row)
    row_buf[...] = row
    for kd in reversed(range(DP)):
        for km in reversed(range(MP)):
            if kd or km:
                pltpu.make_async_remote_copy(
                    src_ref=row_buf, dst_ref=row_slots.at[pl.ds(me, 1)],
                    send_sem=d_send, recv_sem=d_recv,
                    device_id=(dp_peers[kd], mp_peers[km]), device_id_type=MESH,
                ).start()
    row_slots[pl.ds(me, 1), :] = row
    dist_ref[...] = low
    drain(ch_slots, a_send)
    drain(sq_slots, s_send)
    drain(norm_slots, n_send)
    drain(part_slots, b_send)
    others = row_slots.at[pl.ds(0, DP * MP - 1)]
    drain(others, d_send)
    drain(others, d_recv)
    mean_ref[...] = jnp.sum(row_slots[...], axis=0, keepdims=True) / (blk * MP * DP)


def solution(mesh):
    DP, MP = mesh.shape["dp"], mesh.shape["mp"]

    def body(hidden_states, factor_values, class_ids, centers):
        rows, width = hidden_states.shape
        depth = class_ids.shape[1]
        blk = rows // MP
        vm = pltpu.VMEM
        sem = pltpu.SemaphoreType.DMA
        hbm = pl.BlockSpec(memory_space=pl.ANY)
        low, mean = pl.pallas_call(
            functools.partial(kernel, DP, MP),
            out_shape=(vm((1, blk), jnp.float32), vm((1, LANES), jnp.float32)),
            in_specs=[hbm] * 4,
            out_specs=(pl.BlockSpec(memory_space=vm), pl.BlockSpec(memory_space=vm)),
            scratch_shapes=[
                pltpu.SMEM((STEPS,), jnp.int32),
                vm((rows // TALL, TALL, width), jnp.bfloat16),
                vm((rows // LANES, depth, LANES), jnp.bfloat16),
                vm((rows // LANES, depth, LANES), jnp.int32),
                vm((4, width), jnp.bfloat16),
                vm((DP - 1, 4, width), jnp.bfloat16),
                vm((MP, 2, blk), jnp.float32),
                vm((MP - 1, 2, blk), jnp.float32),
                vm((1, LANES), jnp.float32),
                vm((MP - 1, 1, LANES), jnp.float32),
                vm((MP, 2 * STEPS, blk), jnp.float32),
                vm((MP - 1, 2 * STEPS, blk), jnp.float32),
                vm((1, LANES), jnp.float32),
                vm((DP * MP, LANES), jnp.float32),
                *[sem] * 14,
            ],
            compiler_params=pltpu.CompilerParams(collective_id=0, has_side_effects=True),
        )(centers, hidden_states.reshape(rows // TALL, TALL, width), factor_values.T, class_ids.T)
        spec = pl.BlockSpec(memory_space=vm)
        return pl.pallas_call(
            finish,
            out_shape=(
                jax.ShapeDtypeStruct((blk,), jnp.float32),
                jax.ShapeDtypeStruct((STEPS,), jnp.float32),
            ),
            in_specs=[spec, spec],
            out_specs=(spec, spec),
        )(
            pltpu.with_memory_space_constraint(low.reshape(blk), vm),
            pltpu.with_memory_space_constraint(mean.reshape(LANES), vm),
        )

    return jax.shard_map(
        body,
        mesh=mesh,
        in_specs=(P("dp", "mp"), P("dp", "mp"), P("dp", "mp"), P()),
        out_specs=(P(("dp", "mp")), P()),
        check_vma=False,
    )
```
